32 devices in a mesh: cp: 8 (over z, y), tp: 4 (over x, core).
Axes of the slice: x: 2, y: 2, z: 4, core: 2. Of those that a mesh axis runs over, the one named last changes fastest.
Arguments:
- query_rows: bfloat16 [4096, 16384], P(('cp', 'tp')), may hold values from -48 to 48
- token_keys: bfloat16 [4096, 1024], P(('cp', 'tp')), may hold values from -5 to 5
- token_values: bfloat16 [4096, 1024], P(('cp', 'tp')), may hold values from -5 to 5
- doc_lengths: int32 [4], replicated, may hold values from 1 to 2048, 4096 in all
- block_plan: int32 [8, 8], replicated, may hold values from 0 to 7, each once within a row
Outputs:
- attended: bfloat16 [4096, 16384], P(('cp', 'tp'))
The draws below stay inside these ranges and needn't reach their ends.
Inputs may be any that keep to these rules, and one draw needn't show every extreme that they name: `doc_lengths`: the documents fill all 4096 tokens; one of them holds exactly 2048. Each row of block_plan is a permutation of 0 to 7.
All inputs are finite; a program needn't handle non-finite values.
Results may differ from the reference program's by a relative error of at most 0.012.
Values may be sent and summed in bfloat16 or wider, within the bound.
A program may use at most 128 MiB of HBM per device.

```python
import math
import jax
import jax.numpy as jnp
import numpy as np
from jax import lax

QUERY_HEADS_COUNT = 128
KEY_VALUE_HEADS = 8
HEAD_SIZE = 128
TOK_CP = 512
SEQUENCE_TOKENS = 4096
DOC_MOST = 2048
NDOC = 4
SUB = 64
N_CP = 8


def paired_fields(key):
    field_key = jax.random.fold_in(key, 7)
    key_sample, query_draw = jax.random.split(field_key, 2)
    key_random_stream = jnp.clip(jax.random.normal(key_sample, (SEQUENCE_TOKENS, KEY_VALUE_HEADS, HEAD_SIZE), jnp.float32), -5.0, 5.0)
    query_field = jnp.clip(jax.random.normal(query_draw, (SEQUENCE_TOKENS, QUERY_HEADS_COUNT, HEAD_SIZE), jnp.float32), -5.0, 5.0)
    return (query_field, key_random_stream)


def draw_query_rows(key, part):
    query_field, key_random_stream = paired_fields(key)
    return query_field.reshape(SEQUENCE_TOKENS, QUERY_HEADS_COUNT * HEAD_SIZE).astype(jnp.bfloat16)


def draw_token_keys(key, part):
    query_field, key_random_stream = paired_fields(key)
    return key_random_stream.reshape(SEQUENCE_TOKENS, KEY_VALUE_HEADS * HEAD_SIZE).astype(jnp.bfloat16)


def shard_levels(own_key, shape, cuts, low, top_value):
    def one(position, parts):
        heights = jax.random.uniform(jax.random.fold_in(jax.random.fold_in(own_key, 6), position), (parts,), jnp.float32, low / len(cuts), top_value / len(cuts))
        return jnp.repeat(jnp.exp(heights), shape[position] // parts).reshape((-1,) + (1,) * (len(shape) - position - 1))

    level = one(*cuts[0])
    for cut in cuts[1:]:
        level = level * one(*cut)
    return level


def split_up(count, total, most, lean):
    weights = [(1 << 20) // math.isqrt(standing ** lean) + 1 for standing in range(2, count + 1)]
    surplus, holding = total - most - (count - 1), [1] * (count - 1)
    while surplus > 0:
        free = [i for i in range(count - 1) if holding[i] < most]
        whole, remaining = sum([weights[i] for i in free]), surplus
        for i in free:
            addition = min(most - holding[i], max(1, remaining * weights[i] // whole), surplus)
            holding[i] = holding[i] + addition
            surplus = surplus - addition
    return np.array([most] + holding)


def uneven(own_key, amount, total, most, slope):
    if amount == 2:
        one = jax.random.randint(own_key, (), max(1, total - most), min(most, total - 1) + 1)
        return jnp.stack([one, total - one])
    sizes = jnp.asarray(split_up(amount, total, most, slope), jnp.int32)
    pairs = (amount - 1) // 2
    donor, taker = sizes[1:1 + 2 * pairs:2], sizes[2:2 + 2 * pairs:2]
    slack = jnp.minimum(donor - 1, most - taker)
    passed = jax.random.randint(jax.random.fold_in(own_key, 1), (pairs,), 0, 1 << 20) % (slack + 1)
    sizes = sizes.at[1:1 + 2 * pairs:2].set(donor - passed).at[2:2 + 2 * pairs:2].set(taker + passed)
    return sizes[jax.random.permutation(jax.random.fold_in(own_key, 2), amount)]


def gaussian(key, extent, width, bound, shards=(), kind=jnp.bfloat16):
    values = jax.random.normal(key, extent, jnp.float32) * width
    if len(shards) > 0:
        values = shard_levels(key, extent, shards, -0.22, 0.18) * values
    return jnp.clip(values, min=-bound, max=bound).astype(kind)


def setup_inputs(seed: int = 0) -> dict:
    keys = jax.random.split(jax.random.key(seed), 6)
    return {
        "query_rows": draw_query_rows(jax.random.fold_in(keys[5], 71), 0),
        "token_keys": draw_token_keys(jax.random.fold_in(keys[5], 71), 0),
        "token_values": gaussian(keys[2], (SEQUENCE_TOKENS, KEY_VALUE_HEADS * HEAD_SIZE), 1.0, 5.0, ((0, 32),)),
        "doc_lengths": uneven(keys[3], NDOC, SEQUENCE_TOKENS, DOC_MOST, 0).astype(jnp.int32),
        "block_plan": jax.vmap(lambda own: jax.random.permutation(own, N_CP))(jax.random.split(keys[4], N_CP)).reshape((N_CP, N_CP)).astype(jnp.int32),
    }


def scaled_frequencies(head_width):
    exponents = np.arange(0, head_width, 2) / head_width
    inverse = 1.0 / np.power(500000.0, exponents)
    wavelength = 2.0 * np.pi / inverse
    smooth = (8192.0 / wavelength - 1.0) / 3.0
    blended = (1.0 - smooth) * inverse / 8.0 + smooth * inverse
    middle = np.where(wavelength > 8192.0, inverse / 8.0, blended)
    return np.where(wavelength < 2048.0, inverse, middle)

def rotation_tables(head_width, length):
    frequencies = scaled_frequencies(head_width)
    coarse_count = (length + 127) // 128
    coarse_angle = np.arange(coarse_count)[:, None] * 128.0 * frequencies[None, :]
    fine_angle = np.arange(128)[:, None] * 1.0 * frequencies[None, :]
    return (np.cos(coarse_angle), np.sin(coarse_angle), np.cos(fine_angle), np.sin(fine_angle))

def rotation_lookup(positions):
    tables = rotation_tables(HEAD_SIZE, SEQUENCE_TOKENS)
    upper_index = positions // 128
    lower_index = positions % 128
    cosine_high = jnp.asarray(tables[0], jnp.float32)[upper_index]
    sine_high = jnp.asarray(tables[1], jnp.float32)[upper_index]
    cosine_low = jnp.asarray(tables[2], jnp.float32)[lower_index]
    sine_low = jnp.asarray(tables[3], jnp.float32)[lower_index]
    cosine_rows = cosine_high * cosine_low - sine_high * sine_low
    sine_table = sine_high * cosine_low + cosine_high * sine_low
    return (cosine_rows, sine_table)

def apply_rotary_heads(head_rows, cosine_rows, sine_table):
    half_width = head_rows.shape[-1] // 2
    first_half = head_rows[..., :half_width]
    second_half = head_rows[..., half_width:]
    cosine_rows = cosine_rows[:, None, :]
    sine_table = sine_table[:, None, :]
    return jnp.concatenate([first_half * cosine_rows - second_half * sine_table, second_half * cosine_rows + first_half * sine_table], axis=-1)

def attend_exact(query_tile, query_pos, key_window, value_window, key_pos, doc_starts):
    first_pos = lax.optimization_barrier(jnp.max(jnp.where(doc_starts[None, :] <= query_pos[:, None], doc_starts[None, :], 0), axis=1))
    scores = jnp.einsum('rghd,wgd->ghrw', query_tile.astype(jnp.float32), key_window.astype(jnp.float32), precision=lax.Precision.HIGHEST) * (1.0 / math.sqrt(HEAD_SIZE))
    allowed = (key_pos[None, :] <= query_pos[:, None]) & (key_pos[None, :] >= first_pos[:, None])
    masked = jnp.where(allowed, scores, -1e+30)
    highest = lax.optimization_barrier(jnp.max(masked, axis=3, keepdims=True))
    raised = jnp.where(allowed, jnp.exp(masked - highest), 0.0)
    totals = lax.optimization_barrier(jnp.sum(raised, axis=3))
    weights = lax.optimization_barrier(raised.astype(jnp.bfloat16))
    mixed_values = jnp.einsum('ghrw,wgd->rghd', weights.astype(jnp.float32), value_window.astype(jnp.float32), precision=lax.Precision.HIGHEST)
    return (mixed_values / jnp.transpose(totals, (2, 0, 1))[..., None]).astype(jnp.bfloat16)

def reference(query_rows, token_keys, token_values, doc_lengths, block_plan):
    positions = jnp.arange(SEQUENCE_TOKENS, dtype=jnp.int32)
    cosine_rows, sine_table = rotation_lookup(positions)
    doc_starts = (jnp.cumsum(doc_lengths) - doc_lengths).astype(jnp.int32)
    rotary_keys = apply_rotary_heads(token_keys.astype(jnp.float32).reshape(SEQUENCE_TOKENS, KEY_VALUE_HEADS, HEAD_SIZE), cosine_rows, sine_table)
    rotary_keys = lax.optimization_barrier(rotary_keys.astype(jnp.bfloat16))
    grouped_values = token_values.reshape(SEQUENCE_TOKENS, KEY_VALUE_HEADS, HEAD_SIZE)
    block_length = min(256, TOK_CP)
    window_span = DOC_MOST + block_length

    def one_block(block_index):
        block_begin = (block_index * block_length).astype(jnp.int32)
        block_pos = block_begin + jnp.arange(block_length, dtype=jnp.int32)
        block_queries = lax.dynamic_slice_in_dim(query_rows, block_begin, block_length, 0).astype(jnp.float32).reshape(block_length, QUERY_HEADS_COUNT, HEAD_SIZE)
        rotated_heads = apply_rotary_heads(block_queries, lax.dynamic_slice_in_dim(cosine_rows, block_begin, block_length, 0), lax.dynamic_slice_in_dim(sine_table, block_begin, block_length, 0))
        rotated_heads = lax.optimization_barrier(rotated_heads.astype(jnp.bfloat16)).reshape(block_length, KEY_VALUE_HEADS, QUERY_HEADS_COUNT // KEY_VALUE_HEADS, HEAD_SIZE)
        window_begin = jnp.clip(block_begin - DOC_MOST, 0, SEQUENCE_TOKENS - window_span).astype(jnp.int32)
        key_window = lax.dynamic_slice_in_dim(rotary_keys, window_begin, window_span, 0)
        value_window = lax.dynamic_slice_in_dim(grouped_values, window_begin, window_span, 0)
        key_pos = window_begin + jnp.arange(window_span, dtype=jnp.int32)
        return attend_exact(rotated_heads, block_pos, key_window, value_window, key_pos, doc_starts).reshape(block_length, QUERY_HEADS_COUNT * HEAD_SIZE)
    attention = lax.map(one_block, jnp.arange(SEQUENCE_TOKENS // block_length, dtype=jnp.int32)).reshape(SEQUENCE_TOKENS, QUERY_HEADS_COUNT * HEAD_SIZE)
    plan_by_target = jnp.transpose(block_plan).astype(jnp.int32)
    source = jnp.arange(N_CP, dtype=jnp.int32)[None, :, None] * TOK_CP + plan_by_target[:, :, None] * SUB + jnp.arange(SUB, dtype=jnp.int32)[None, None, :]
    return attention[source.reshape(-1)]
```

```python
import functools
import math

import jax
import jax.numpy as jnp
import numpy as np
from jax import lax
from jax.experimental import pallas as pl
from jax.experimental.pallas import tpu as pltpu
from jax.sharding import PartitionSpec as P

HEAD_SIZE = 128
DOC_MOST = 2048


def shifted(x, axis, by):
    peers = lax.axis_size(axis)
    pairs = [(i, i + by) for i in range(peers) if 0 <= i + by < peers]
    return lax.ppermute(x, axis, pairs)


def scaled_frequencies(head_width):
    exponents = np.arange(0, head_width, 2) / head_width
    inverse = 1.0 / np.power(500000.0, exponents)
    wavelength = 2.0 * np.pi / inverse
    smooth = (8192.0 / wavelength - 1.0) / 3.0
    blended = (1.0 - smooth) * inverse / 8.0 + smooth * inverse
    middle = np.where(wavelength > 8192.0, inverse / 8.0, blended)
    return np.where(wavelength < 2048.0, inverse, middle)


def rotation_tables(head_width, length):
    frequencies = scaled_frequencies(head_width)
    coarse_count = (length + 127) // 128
    coarse_angle = np.arange(coarse_count)[:, None] * 128.0 * frequencies[None, :]
    fine_angle = np.arange(128)[:, None] * 1.0 * frequencies[None, :]
    return (np.cos(coarse_angle), np.sin(coarse_angle), np.cos(fine_angle), np.sin(fine_angle))


def rotation_rows(positions, head_width, length):
    tables = rotation_tables(head_width, length)
    coarse_count = tables[0].shape[0]
    upper_hit = (
        (positions // 128)[:, None] == jnp.arange(coarse_count, dtype=jnp.int32)[None, :]
    ).astype(jnp.float32)
    lower_hit = ((positions % 128)[:, None] == jnp.arange(128, dtype=jnp.int32)[None, :]).astype(
        jnp.float32
    )
    picked = []
    for lookup_table, selector in zip(tables, (upper_hit, upper_hit, lower_hit, lower_hit)):
        picked.append(
            jnp.dot(
                selector, jnp.asarray(lookup_table, jnp.float32), precision=lax.Precision.HIGHEST
            )
        )
    cosine_rows = picked[0] * picked[2] - picked[1] * picked[3]
    sine_table = picked[1] * picked[2] + picked[0] * picked[3]
    return (cosine_rows, sine_table)


def apply_rotary_heads(head_rows, cosine_rows, sine_table):
    half_width = head_rows.shape[-1] // 2
    first_half = head_rows[..., :half_width]
    second_half = head_rows[..., half_width:]
    cosine_rows = cosine_rows[:, None, :]
    sine_table = sine_table[:, None, :]
    return jnp.concatenate(
        [
            first_half * cosine_rows - second_half * sine_table,
            second_half * cosine_rows + first_half * sine_table,
        ],
        axis=-1,
    )


def attend_and_place(cp_count, tp_count, shape, plan_ref, query_ref, cosine_ref, sine_ref, mark_ref,
                     key_ref, value_ref, out_ref, outbox, send_sem, recv_sem, own_sem):
    block_rows, sub_rows, groups, per_group, window = shape
    cp_index = lax.axis_index("cp")
    tp_index = lax.axis_index("tp")
    held = cp_count // tp_count
    width = per_group * HEAD_SIZE
    target_tp = cp_index // held
    sub_here = cp_index % held
    steps = cp_count * groups
    batch = max(1, min(per_group, 512 // sub_rows))
    tile = batch * sub_rows
    past = window - sub_rows

    def target_of(order):
        if cp_count % 2:
            return lax.rem(cp_index + order, cp_count)
        half = cp_count // 2
        side = lax.rem(cp_index // half + 1 + order // half, 2)
        return side * half + lax.rem(cp_index + order, half)

    def remote(step, target_cp):
        group = lax.rem(step, groups)
        column = pl.multiple_of((tp_index * groups + group) * width, width)
        row = pl.multiple_of(sub_here * sub_rows, sub_rows)
        slot = (sub_here * tp_count + tp_index) * groups + group
        return pltpu.make_async_remote_copy(
            src_ref=outbox.at[step],
            dst_ref=out_ref.at[pl.ds(row, sub_rows), pl.ds(column, width)],
            send_sem=send_sem.at[step],
            recv_sem=recv_sem.at[slot],
            device_id=(target_cp, target_tp),
            device_id_type=pl.DeviceIdType.MESH,
        )

    def local(step):
        group = lax.rem(step, groups)
        column = pl.multiple_of((tp_index * groups + group) * width, width)
        row = pl.multiple_of(sub_here * sub_rows, sub_rows)
        return pltpu.make_async_copy(
            outbox.at[step],
            out_ref.at[pl.ds(row, sub_rows), pl.ds(column, width)],
            own_sem.at[group],
        )

    def is_self(target_cp):
        return jnp.logical_and(target_cp == cp_index, target_tp == tp_index)

    def one_step(step, carry):
        order = step // groups
        group = lax.rem(step, groups)
        target_cp = target_of(order)
        piece = plan_ref[cp_index, target_cp]
        cosine = cosine_ref[piece]
        sine = sine_ref[piece]
        mark = mark_ref[piece]
        reach = window // sub_rows
        keys = key_ref[group, pl.ds(piece, reach)].reshape(window, 2 * HEAD_SIZE)
        values = value_ref[group, pl.ds(piece, reach)].reshape(window, HEAD_SIZE)
        causal = lax.broadcasted_iota(jnp.int32, (sub_rows, sub_rows), 1) <= lax.broadcasted_iota(
            jnp.int32, (sub_rows, sub_rows), 0
        )
        causal_all = jnp.concatenate([causal.astype(jnp.float32)] * batch, axis=0) > 0.5
        for part in range(per_group // batch):
            rotated = []
            for head in range(batch):
                column = pl.multiple_of(group * width, width) + (part * batch + head) * HEAD_SIZE
                column = pl.multiple_of(column, HEAD_SIZE)
                raw = query_ref[piece, :, pl.ds(column, HEAD_SIZE)].astype(jnp.float32)
                turned = raw * cosine + pltpu.roll(raw, HEAD_SIZE // 2, 1) * sine
                rotated.append(jnp.concatenate([turned.astype(jnp.bfloat16), mark], axis=1))
            queries = jnp.concatenate(rotated, axis=0)
            nt = (((1,), (1,)), ((), ()))
            early = lax.dot_general(queries, keys[:past], nt, preferred_element_type=jnp.float32)
            late = lax.dot_general(queries, keys[past:], nt, preferred_element_type=jnp.float32)
            late = jnp.where(causal_all, late, -1e30)
            highest = jnp.maximum(
                jnp.max(early, axis=1, keepdims=True), jnp.max(late, axis=1, keepdims=True)
            )
            early = jnp.exp2(early - highest)
            late = jnp.exp2(late - highest)
            totals = jnp.sum(early, axis=1, keepdims=True) + jnp.sum(late, axis=1, keepdims=True)
            mixed = jnp.dot(early.astype(jnp.bfloat16), values[:past], preferred_element_type=jnp.float32)
            mixed += jnp.dot(late.astype(jnp.bfloat16), values[past:], preferred_element_type=jnp.float32)
            result = (mixed / totals).astype(jnp.bfloat16)
            for head in range(batch):
                column = (part * batch + head) * HEAD_SIZE
                outbox[step, :, column:column + HEAD_SIZE] = result[head * sub_rows:(head + 1) * sub_rows]
        own = is_self(target_cp)

        @pl.when(jnp.logical_not(own))
        def _():
            remote(step, target_cp).start()

        @pl.when(own)
        def _():
            local(step).start()

        return carry

    lax.fori_loop(0, steps, one_step, 0)

    def finish(step, carry):
        target_cp = target_of(step // groups)
        own = is_self(target_cp)

        @pl.when(jnp.logical_not(own))
        def _():
            remote(step, target_cp).wait_send()

        @pl.when(own)
        def _():
            local(step).wait()

        return carry

    lax.fori_loop(0, steps, finish, 0)

    def arrive(slot, carry):
        group = lax.rem(slot, groups)
        from_tp = lax.rem(slot // groups, tp_count)
        from_sub = slot // (groups * tp_count)
        from_cp = tp_index * held + from_sub

        @pl.when(jnp.logical_not(jnp.logical_and(from_cp == cp_index, from_tp == tp_index)))
        def _():
            column = pl.multiple_of((from_tp * groups + group) * width, width)
            row = pl.multiple_of(from_sub * sub_rows, sub_rows)
            pltpu.make_async_remote_copy(
                src_ref=outbox.at[0],
                dst_ref=out_ref.at[pl.ds(row, sub_rows), pl.ds(column, width)],
                send_sem=send_sem.at[0],
                recv_sem=recv_sem.at[slot],
                device_id=(from_cp, from_tp),
                device_id_type=pl.DeviceIdType.MESH,
            ).wait_recv()

        return carry

    lax.fori_loop(0, held * tp_count * groups, arrive, 0)


def on_device(query_rows, token_keys, token_values, doc_lengths, block_plan):
    query_heads, key_heads, value_heads = (
        lax.all_to_all(query_rows, "tp", split_axis=1, concat_axis=0, tiled=True),
        lax.all_to_all(token_keys, "tp", split_axis=1, concat_axis=0, tiled=True),
        lax.all_to_all(token_values, "tp", split_axis=1, concat_axis=0, tiled=True),
    )
    block_rows = query_heads.shape[0]
    cp_count = lax.axis_size("cp")
    tp_count = lax.axis_size("tp")
    cp_index = lax.axis_index("cp")
    sequence = block_rows * cp_count
    sub_rows = block_rows // cp_count
    groups = key_heads.shape[1] // HEAD_SIZE
    per_group = query_heads.shape[1] // HEAD_SIZE // groups
    positions = cp_index * block_rows + jnp.arange(block_rows, dtype=jnp.int32)
    cosine_rows, sine_table = rotation_rows(positions, HEAD_SIZE, sequence)
    rotary_keys = apply_rotary_heads(
        key_heads.astype(jnp.float32).reshape(block_rows, groups, HEAD_SIZE), cosine_rows, sine_table
    ).astype(jnp.bfloat16)
    packed = jnp.concatenate([rotary_keys.reshape(block_rows, groups * HEAD_SIZE), value_heads], axis=1)
    reach_blocks = DOC_MOST // block_rows
    earlier = [shifted(packed, "cp", distance) for distance in range(reach_blocks, 0, -1)]
    window_rows = jnp.concatenate(earlier + [packed], axis=0)
    window_pos = (cp_index - reach_blocks) * block_rows + jnp.arange(
        (reach_blocks + 1) * block_rows, dtype=jnp.int32
    )
    doc_ends = jnp.cumsum(doc_lengths)
    lanes = jnp.arange(HEAD_SIZE, dtype=jnp.int32)[None, :]

    def document(pos):
        index = jnp.sum((doc_ends[None, :] <= pos[:, None]).astype(jnp.int32), axis=1)
        return jnp.where(pos < 0, HEAD_SIZE - 1, index)[:, None]

    key_marks = (document(window_pos) == lanes).astype(jnp.bfloat16)
    query_marks = jnp.where(document(positions) == lanes, 0.0, -1e30).astype(jnp.bfloat16)
    window_keys = jnp.stack(
        [
            jnp.concatenate([window_rows[:, g * HEAD_SIZE:(g + 1) * HEAD_SIZE], key_marks], axis=1)
            for g in range(groups)
        ]
    )
    window_values = jnp.stack(
        [window_rows[:, (groups + g) * HEAD_SIZE:(groups + g + 1) * HEAD_SIZE] for g in range(groups)]
    )
    scale = math.log2(math.e) / math.sqrt(HEAD_SIZE)
    cosine_wide = jnp.concatenate([cosine_rows, cosine_rows], axis=1) * scale
    sine_wide = jnp.concatenate([-sine_table, sine_table], axis=1) * scale
    window = DOC_MOST + sub_rows
    steps = cp_count * groups
    width = per_group * HEAD_SIZE
    vmem = pl.BlockSpec(memory_space=pltpu.VMEM)
    return pl.pallas_call(
        functools.partial(
            attend_and_place, cp_count, tp_count, (block_rows, sub_rows, groups, per_group, window)
        ),
        out_shape=jax.ShapeDtypeStruct(query_rows.shape, jnp.bfloat16),
        in_specs=[pl.BlockSpec(memory_space=pltpu.SMEM)] + [vmem] * 6,
        out_specs=pl.BlockSpec(memory_space=pl.ANY),
        scratch_shapes=[
            pltpu.VMEM((steps, sub_rows, width), jnp.bfloat16),
            pltpu.SemaphoreType.DMA((steps,)),
            pltpu.SemaphoreType.DMA((steps,)),
            pltpu.SemaphoreType.DMA((groups,)),
        ],
        compiler_params=pltpu.CompilerParams(has_side_effects=True, vmem_limit_bytes=60 * 2**20),
    )(
        block_plan,
        query_heads.reshape(cp_count, sub_rows, -1),
        cosine_wide.reshape(cp_count, sub_rows, -1),
        sine_wide.reshape(cp_count, sub_rows, -1),
        query_marks.reshape(cp_count, sub_rows, -1),
        window_keys.reshape(groups, -1, sub_rows, 2 * HEAD_SIZE),
        window_values.reshape(groups, -1, sub_rows, HEAD_SIZE),
    )


def solution(mesh):
    placed = (P(("cp", "tp"), None), P(("cp", "tp"), None), P(("cp", "tp"), None), P(), P())
    return jax.shard_map(
        on_device, mesh=mesh, in_specs=placed, out_specs=P(("cp", "tp"), None), check_vma=False
    )
```

```python
import functools
import math

import jax
import jax.numpy as jnp
import numpy as np
from jax import lax
from jax.experimental import pallas as pl
from jax.experimental.pallas import tpu as pltpu
from jax.sharding import PartitionSpec as P

HEAD_SIZE = 128
DOC_MOST = 2048


def shifted(x, axis, by):
    peers = lax.axis_size(axis)
    pairs = [(i, i + by) for i in range(peers) if 0 <= i + by < peers]
    return lax.ppermute(x, axis, pairs)


def scaled_frequencies(head_width):
    exponents = np.arange(0, head_width, 2) / head_width
    inverse = 1.0 / np.power(500000.0, exponents)
    wavelength = 2.0 * np.pi / inverse
    smooth = (8192.0 / wavelength - 1.0) / 3.0
    blended = (1.0 - smooth) * inverse / 8.0 + smooth * inverse
    middle = np.where(wavelength > 8192.0, inverse / 8.0, blended)
    return np.where(wavelength < 2048.0, inverse, middle)


def rotation_tables(head_width, length):
    frequencies = scaled_frequencies(head_width)
    coarse_count = (length + 127) // 128
    coarse_angle = np.arange(coarse_count)[:, None] * 128.0 * frequencies[None, :]
    fine_angle = np.arange(128)[:, None] * 1.0 * frequencies[None, :]
    return (np.cos(coarse_angle), np.sin(coarse_angle), np.cos(fine_angle), np.sin(fine_angle))


def rotation_rows(positions, head_width, length):
    tables = rotation_tables(head_width, length)
    coarse_count = tables[0].shape[0]
    upper_hit = (
        (positions // 128)[:, None] == jnp.arange(coarse_count, dtype=jnp.int32)[None, :]
    ).astype(jnp.float32)
    lower_hit = ((positions % 128)[:, None] == jnp.arange(128, dtype=jnp.int32)[None, :]).astype(
        jnp.float32
    )
    picked = []
    for lookup_table, selector in zip(tables, (upper_hit, upper_hit, lower_hit, lower_hit)):
        picked.append(
            jnp.dot(
                selector, jnp.asarray(lookup_table, jnp.float32), precision=lax.Precision.HIGHEST
            )
        )
    cosine_rows = picked[0] * picked[2] - picked[1] * picked[3]
    sine_table = picked[1] * picked[2] + picked[0] * picked[3]
    return (cosine_rows, sine_table)


def apply_rotary_heads(head_rows, cosine_rows, sine_table):
    half_width = head_rows.shape[-1] // 2
    first_half = head_rows[..., :half_width]
    second_half = head_rows[..., half_width:]
    cosine_rows = cosine_rows[:, None, :]
    sine_table = sine_table[:, None, :]
    return jnp.concatenate(
        [
            first_half * cosine_rows - second_half * sine_table,
            second_half * cosine_rows + first_half * sine_table,
        ],
        axis=-1,
    )


def attend_and_place(cp_count, tp_count, shape, plan_ref, query_ref, cosine_ref, sine_ref, mark_ref,
                     key_ref, value_ref, out_ref, outbox, send_sem, recv_sem, own_sem):
    block_rows, sub_rows, groups, per_group, window = shape
    cp_index = lax.axis_index("cp")
    tp_index = lax.axis_index("tp")
    held = cp_count // tp_count
    width = per_group * HEAD_SIZE
    target_tp = cp_index // held
    sub_here = cp_index % held
    steps = cp_count * groups
    batch = max(1, min(per_group, 512 // sub_rows))
    tile = batch * sub_rows
    past = window - sub_rows

    def target_of(order):
        if cp_count % 4:
            return lax.rem(cp_index + order, cp_count)
        half = cp_count // 2
        quarter = cp_count // 4
        mine = cp_index // quarter
        outer = 1 - ((mine + 1) // 2) % 2
        near_first = jnp.where(
            order < quarter, order + half, jnp.where(order < half + quarter, order - quarter, order)
        )
        place = jnp.where(outer == 1, near_first, order)
        across = (1 - cp_index // half) * half + (cp_index + place) % half
        beside = (mine // 2 * 2 + 1 - mine % 2) * quarter + (cp_index + place) % quarter
        within = mine * quarter + (cp_index + 1 + place) % quarter
        return jnp.where(place < half, across, jnp.where(place < half + quarter, beside, within))

    def remote(step, target_cp):
        group = lax.rem(step, groups)
        column = pl.multiple_of((tp_index * groups + group) * width, width)
        row = pl.multiple_of(sub_here * sub_rows, sub_rows)
        slot = (sub_here * tp_count + tp_index) * groups + group
        return pltpu.make_async_remote_copy(
            src_ref=outbox.at[step],
            dst_ref=out_ref.at[pl.ds(row, sub_rows), pl.ds(column, width)],
            send_sem=send_sem.at[step],
            recv_sem=recv_sem.at[slot],
            device_id=(target_cp, target_tp),
            device_id_type=pl.DeviceIdType.MESH,
        )

    def local(step):
        group = lax.rem(step, groups)
        column = pl.multiple_of((tp_index * groups + group) * width, width)
        row = pl.multiple_of(sub_here * sub_rows, sub_rows)
        return pltpu.make_async_copy(
            outbox.at[step],
            out_ref.at[pl.ds(row, sub_rows), pl.ds(column, width)],
            own_sem.at[group],
        )

    def is_self(target_cp):
        return jnp.logical_and(target_cp == cp_index, target_tp == tp_index)

    def one_step(step, carry):
        order = step // groups
        group = lax.rem(step, groups)
        target_cp = target_of(order)
        piece = plan_ref[cp_index, target_cp]
        cosine = cosine_ref[piece]
        sine = sine_ref[piece]
        mark = mark_ref[piece]
        reach = window // sub_rows
        keys = key_ref[group, pl.ds(piece, reach)].reshape(window, 2 * HEAD_SIZE)
        values = value_ref[group, pl.ds(piece, reach)].reshape(window, HEAD_SIZE)
        causal = lax.broadcasted_iota(jnp.int32, (sub_rows, sub_rows), 1) <= lax.broadcasted_iota(
            jnp.int32, (sub_rows, sub_rows), 0
        )
        causal_all = jnp.concatenate([causal.astype(jnp.float32)] * batch, axis=0) > 0.5
        for part in range(per_group // batch):
            rotated = []
            for head in range(batch):
                column = pl.multiple_of(group * width, width) + (part * batch + head) * HEAD_SIZE
                column = pl.multiple_of(column, HEAD_SIZE)
                raw = query_ref[piece, :, pl.ds(column, HEAD_SIZE)].astype(jnp.float32)
                turned = raw * cosine + pltpu.roll(raw, HEAD_SIZE // 2, 1) * sine
                rotated.append(jnp.concatenate([turned.astype(jnp.bfloat16), mark], axis=1))
            queries = jnp.concatenate(rotated, axis=0)
            nt = (((1,), (1,)), ((), ()))
            early = lax.dot_general(queries, keys[:past], nt, preferred_element_type=jnp.float32)
            late = lax.dot_general(queries, keys[past:], nt, preferred_element_type=jnp.float32)
            late = jnp.where(causal_all, late, -1e30)
            highest = jnp.maximum(
                jnp.max(early, axis=1, keepdims=True), jnp.max(late, axis=1, keepdims=True)
            )
            early = jnp.exp2(early - highest)
            late = jnp.exp2(late - highest)
            totals = jnp.sum(early, axis=1, keepdims=True) + jnp.sum(late, axis=1, keepdims=True)
            mixed = jnp.dot(early.astype(jnp.bfloat16), values[:past], preferred_element_type=jnp.float32)
            mixed += jnp.dot(late.astype(jnp.bfloat16), values[past:], preferred_element_type=jnp.float32)
            result = (mixed / totals).astype(jnp.bfloat16)
            for head in range(batch):
                column = (part * batch + head) * HEAD_SIZE
                outbox[step, :, column:column + HEAD_SIZE] = result[head * sub_rows:(head + 1) * sub_rows]
        own = is_self(target_cp)

        @pl.when(jnp.logical_not(own))
        def _():
            remote(step, target_cp).start()

        @pl.when(own)
        def _():
            local(step).start()

        return carry

    lax.fori_loop(0, steps, one_step, 0)

    def finish(step, carry):
        target_cp = target_of(step // groups)
        own = is_self(target_cp)

        @pl.when(jnp.logical_not(own))
        def _():
            remote(step, target_cp).wait_send()

        @pl.when(own)
        def _():
            local(step).wait()

        return carry

    lax.fori_loop(0, steps, finish, 0)

    def arrive(slot, carry):
        group = lax.rem(slot, groups)
        from_tp = lax.rem(slot // groups, tp_count)
        from_sub = slot // (groups * tp_count)
        from_cp = tp_index * held + from_sub

        @pl.when(jnp.logical_not(jnp.logical_and(from_cp == cp_index, from_tp == tp_index)))
        def _():
            column = pl.multiple_of((from_tp * groups + group) * width, width)
            row = pl.multiple_of(from_sub * sub_rows, sub_rows)
            pltpu.make_async_remote_copy(
                src_ref=outbox.at[0],
                dst_ref=out_ref.at[pl.ds(row, sub_rows), pl.ds(column, width)],
                send_sem=send_sem.at[0],
                recv_sem=recv_sem.at[slot],
                device_id=(from_cp, from_tp),
                device_id_type=pl.DeviceIdType.MESH,
            ).wait_recv()

        return carry

    lax.fori_loop(0, held * tp_count * groups, arrive, 0)


def on_device(query_rows, token_keys, token_values, doc_lengths, block_plan):
    tp_count = lax.axis_size("tp")
    own_rows = token_keys.shape[0]
    paired = jnp.concatenate(
        [token_keys.reshape(own_rows, tp_count, -1), token_values.reshape(own_rows, tp_count, -1)], axis=2
    ).reshape(own_rows, -1)
    paired_heads = lax.all_to_all(paired, "tp", split_axis=1, concat_axis=0, tiled=True)
    query_heads = lax.all_to_all(query_rows, "tp", split_axis=1, concat_axis=0, tiled=True)
    key_heads = paired_heads[:, : paired_heads.shape[1] // 2]
    value_heads = paired_heads[:, paired_heads.shape[1] // 2 :]
    block_rows = query_heads.shape[0]
    cp_count = lax.axis_size("cp")
    cp_index = lax.axis_index("cp")
    sequence = block_rows * cp_count
    sub_rows = block_rows // cp_count
    groups = key_heads.shape[1] // HEAD_SIZE
    per_group = query_heads.shape[1] // HEAD_SIZE // groups
    positions = cp_index * block_rows + jnp.arange(block_rows, dtype=jnp.int32)
    cosine_rows, sine_table = rotation_rows(positions, HEAD_SIZE, sequence)
    rotary_keys = apply_rotary_heads(
        key_heads.astype(jnp.float32).reshape(block_rows, groups, HEAD_SIZE), cosine_rows, sine_table
    ).astype(jnp.bfloat16)
    packed = jnp.concatenate([rotary_keys.reshape(block_rows, groups * HEAD_SIZE), value_heads], axis=1)
    reach_blocks = DOC_MOST // block_rows
    blocks = [packed]
    for distance in range(1, reach_blocks + 1):
        step = min(2, distance)
        blocks.append(shifted(blocks[distance - step], "cp", step))
    window_rows = jnp.concatenate(blocks[::-1], axis=0)
    window_pos = (cp_index - reach_blocks) * block_rows + jnp.arange(
        (reach_blocks + 1) * block_rows, dtype=jnp.int32
    )
    doc_ends = jnp.cumsum(doc_lengths)
    lanes = jnp.arange(HEAD_SIZE, dtype=jnp.int32)[None, :]

    def document(pos):
        index = jnp.sum((doc_ends[None, :] <= pos[:, None]).astype(jnp.int32), axis=1)
        return jnp.where(pos < 0, HEAD_SIZE - 1, index)[:, None]

    key_marks = (document(window_pos) == lanes).astype(jnp.bfloat16)
    query_marks = jnp.where(document(positions) == lanes, 0.0, -1e30).astype(jnp.bfloat16)
    window_keys = jnp.stack(
        [
            jnp.concatenate([window_rows[:, g * HEAD_SIZE:(g + 1) * HEAD_SIZE], key_marks], axis=1)
            for g in range(groups)
        ]
    )
    window_values = jnp.stack(
        [window_rows[:, (groups + g) * HEAD_SIZE:(groups + g + 1) * HEAD_SIZE] for g in range(groups)]
    )
    scale = math.log2(math.e) / math.sqrt(HEAD_SIZE)
    cosine_wide = jnp.concatenate([cosine_rows, cosine_rows], axis=1) * scale
    sine_wide = jnp.concatenate([-sine_table, sine_table], axis=1) * scale
    window = DOC_MOST + sub_rows
    steps = cp_count * groups
    width = per_group * HEAD_SIZE
    vmem = pl.BlockSpec(memory_space=pltpu.VMEM)
    return pl.pallas_call(
        functools.partial(
            attend_and_place, cp_count, tp_count, (block_rows, sub_rows, groups, per_group, window)
        ),
        out_shape=jax.ShapeDtypeStruct(query_rows.shape, jnp.bfloat16),
        in_specs=[pl.BlockSpec(memory_space=pltpu.SMEM)] + [vmem] * 6,
        out_specs=pl.BlockSpec(memory_space=pl.ANY),
        scratch_shapes=[
            pltpu.VMEM((steps, sub_rows, width), jnp.bfloat16),
            pltpu.SemaphoreType.DMA((steps,)),
            pltpu.SemaphoreType.DMA((steps,)),
            pltpu.SemaphoreType.DMA((groups,)),
        ],
        compiler_params=pltpu.CompilerParams(has_side_effects=True, vmem_limit_bytes=60 * 2**20),
    )(
        block_plan,
        query_heads.reshape(cp_count, sub_rows, -1),
        cosine_wide.reshape(cp_count, sub_rows, -1),
        sine_wide.reshape(cp_count, sub_rows, -1),
        query_marks.reshape(cp_count, sub_rows, -1),
        window_keys.reshape(groups, -1, sub_rows, 2 * HEAD_SIZE),
        window_values.reshape(groups, -1, sub_rows, HEAD_SIZE),
    )


def solution(mesh):
    placed = (P(("cp", "tp"), None), P(("cp", "tp"), None), P(("cp", "tp"), None), P(), P())
    return jax.shard_map(
        on_device, mesh=mesh, in_specs=placed, out_specs=P(("cp", "tp"), None), check_vma=False
    )
```
